32 devices in a mesh: row: 8 (over z, core), col: 4 (over y, x).
Axes of the slice: x: 2, y: 2, z: 4, core: 2. Of those that a mesh axis runs over, the one named last changes fastest.
Arguments:
- factor: bfloat16 [8192, 8192], P('row', 'col'), as said below
- sel_tiles: int32 [32], replicated, may hold values from 0 to 63, as said below
- coupling: bfloat16 [8192, 2048], P('col', 'row')
Outputs:
- root_inverse: float32 [8192, 8192], P('row', 'col')
- child_inverse: float32 [2048, 8192], P('col', 'row')
The draws below stay inside these ranges and needn't reach their ends.
Inputs may be any that keep to these rules, and one draw needn't show every extreme that they name: sel_tiles holds 32 distinct tile indices in increasing order; rows of coupling outside the listed tiles are zero. factor is lower triangular with a diagonal between 1 and 1.5.
All inputs are finite; a program needn't handle non-finite values.
Results may differ from the reference program's by a relative error of at most 0.003.
Values may be sent and summed in bfloat16 or wider, within the bound.
No kernel may reach another device: no remote copies, remote signals or barrier semaphores. Data moves between devices by JAX's collectives and lax.ppermute only.
A program may use at most 128 MiB of HBM per device.

```python
import jax
import jax.numpy as jnp

S = 8192
TILE = 128
NCH = 2048
R = 32


def chosen_tiles(key):
    order = jax.random.permutation(jax.random.fold_in(key, 7), S // TILE)
    return jnp.sort(order[:R]).astype(jnp.int32)


def draw_sel_tiles(key, part):
    return chosen_tiles(key)


def draw_factor(key, part):
    first = jax.random.fold_in(key, 11)
    second = jax.random.fold_in(key, 13)
    rows = jnp.arange(S)[:, None]
    cols = jnp.arange(S)[None, :]
    lower = jax.random.normal(first, (S, S), jnp.float32)
    lower = lower * S ** (-0.5)
    diag = 1.0 + 0.5 * jax.random.uniform(second, (S,), jnp.float32)
    full = jnp.where(rows > cols, lower, 0.0) + jnp.where(rows == cols, diag[None, :], 0.0)
    return full.astype(jnp.bfloat16)


def draw_coupling(key, part):
    tiles = chosen_tiles(key)
    tile_of = (jnp.arange(S) // TILE).astype(jnp.int32)
    member = jnp.any(tile_of[:, None] == tiles[None, :], axis=1)
    values = 0.5 * jax.random.normal(jax.random.fold_in(key, 5), (S, NCH), jnp.float32)
    return jnp.where(member[:, None], values, 0.0).astype(jnp.bfloat16)


def setup_inputs(seed: int = 0) -> dict:
    key_of = jax.random.split(jax.random.key(seed), 4)
    factor = draw_factor(jax.random.fold_in(key_of[3], 71), 0)
    sel_tiles = draw_sel_tiles(jax.random.fold_in(key_of[3], 71), 0)
    coupling = draw_coupling(jax.random.fold_in(key_of[3], 71), 0)
    return {"factor": factor, "sel_tiles": sel_tiles, "coupling": coupling}


def reference(factor, sel_tiles, coupling):
    gram = jnp.dot(factor.T, factor, preferred_element_type=jnp.float32)
    rounded = gram.astype(jnp.bfloat16)
    tile_of = (jnp.arange(S) // TILE).astype(jnp.int32)
    member = jnp.any(tile_of[:, None] == sel_tiles[None, :], axis=1)
    product = jnp.dot(coupling.T, rounded.T, preferred_element_type=jnp.float32)
    child = jnp.where(member[None, :], -product, jnp.float32(0.0))
    return gram, child
```

```python
import jax
import jax.numpy as jnp
from jax import lax
from jax.sharding import PartitionSpec as P

TILE = 128
CORES = 2
CHUNKS = 2


def dot_f32(a, b, dims):
    return lax.dot_general(a, b, (dims, ((), ())), preferred_element_type=jnp.float32)


def member_of(sel_tiles, row_index, rows_here):
    rows = row_index * rows_here + jnp.arange(rows_here, dtype=jnp.int32)
    return jnp.any((rows // TILE)[:, None] == sel_tiles[None, :], axis=1)


def from_root(value, axis, source):
    kept = jnp.where(lax.axis_index(axis) == source, value, 0).astype(value.dtype)
    return lax.psum(kept, axis)


def general_body(factor, sel_tiles, coupling):
    rows_here = factor.shape[0]
    row_index = lax.axis_index("row")
    whole = lax.all_gather(factor, "row", axis=0, tiled=True)
    ratio = lax.axis_size("row") // lax.axis_size("col")
    offset = row_index % ratio * rows_here
    piece = lax.dynamic_slice_in_dim(whole, offset, rows_here, 1)
    partner = from_root(piece, "col", row_index // ratio)
    gram = dot_f32(partner, whole, ((0,), (0,)))
    coupling_full = lax.all_gather(coupling, "row", axis=1, tiled=True)
    rounded = gram.astype(jnp.bfloat16)
    member = member_of(sel_tiles, row_index, rows_here)
    summed = lax.psum_scatter(
        dot_f32(coupling_full, rounded, ((0,), (1,))), "col", scatter_dimension=0, tiled=True
    )
    child = jnp.where(member[None, :], -summed, jnp.float32(0.0))
    return (gram, child)


def square_body(factor, sel_tiles, coupling):
    rows_here, cols_here = factor.shape
    cols = lax.axis_size("col")
    planes = lax.axis_size("row") // CORES
    row_index = lax.axis_index("row")
    col_index = lax.axis_index("col")
    plane, core = row_index // CORES, row_index % CORES
    step = rows_here // CHUNKS

    def along_z(value, moves):
        pairs = [(CORES * s + k, CORES * t + k) for s, t in moves for k in range(CORES)]
        return lax.ppermute(value, "row", pairs)

    def swap_core(value):
        pairs = [(r, r ^ 1) for r in range(CORES * planes)]
        return lax.ppermute(value, "row", pairs)

    def in_plane(value, source, target, z_list):
        pairs = []
        for z in z_list:
            for k in range(CORES):
                r = CORES * z + k
                pairs.append((r * cols + (z ^ source), r * cols + (z ^ target)))
        return lax.ppermute(value, ("row", "col"), pairs)

    is_root = col_index == plane

    last = planes - 1
    half = cols_here // CORES
    down = [(z, z - 1) for z in range(1, planes)]
    blocks = {(0, k): factor[k * step : (k + 1) * step] for k in range(CHUNKS)}
    hops = {}
    arrival = {(0, 0): 0, (0, 1): 0, (1, 0): 1, (3, 1): 1, (1, 1): 2, (3, 0): 2, (2, 0): 3, (2, 1): 4}
    parts = {}

    def dot_of(keys):
        left, right = [], []
        for key in keys:
            left += [parts[key], hops["t", key]]
            right += [blocks[key], hops["s", key]]
        return dot_f32(jnp.concatenate(left, 0), jnp.concatenate(right, 0), ((0,), (0,)))

    dots_at = {5: [(0, 0), (0, 1)], 6: [(1, 0), (3, 1)]}
    gram = jnp.zeros((), jnp.float32)
    for step_no in range(1, 8):
        got = {}
        if step_no in dots_at:
            gram = gram + dot_of(dots_at[step_no])
        for key, when in arrival.items():
            d, k = key
            if when == step_no:
                if d == 1:
                    got["z", key] = along_z(blocks[0, k], down)
                elif d == 3:
                    got["z", key] = along_z(blocks[0, k], [(last, 0)])
                else:
                    relay = jnp.where(plane == 0, blocks[3, k], blocks[1, k])
                    got["z", key] = along_z(relay, [(1, 0), (0, 1)])
            z_list = [z for z in range(planes) if z + d < planes and z + d > 0]
            first, second = (1, 2) if k == 0 else (2, 1)
            age = step_no - when
            if age == 1:
                got["a", key] = in_plane(blocks[key], 0, first, z_list)
                got["s", key] = swap_core(blocks[key])
                if d == 2:
                    got["c", key] = in_plane(blocks[key], 0, second, z_list)
            elif age == 2:
                got["b", key] = in_plane(hops["a", key], first, 3, z_list)
            elif age == 3 and d != 2:
                got["c", key] = in_plane(hops["b", key], 3, second, z_list)
            if age == (3 if d == 2 else 4):
                moved = hops["a", key] + hops["b", key] + hops["c", key]
                part = jnp.where(is_root, blocks[key], moved)
                parts[key] = lax.dynamic_slice_in_dim(part, core * half, half, 1)
                theirs = lax.dynamic_slice_in_dim(part, (1 - core) * half, half, 1)
                got["t", key] = swap_core(theirs)
        names = list(got)
        keep = list(blocks)
        values, kept, gram, coupling = lax.optimization_barrier(
            ([got[n] for n in names], [blocks[n] for n in keep], gram, coupling)
        )
        if step_no == 4:
            coupling_full = lax.all_gather(coupling, "row", axis=1, tiled=True)
        blocks = dict(zip(keep, kept))
        for name, value in zip(names, values):
            if name[0] == "z":
                blocks[name[1]] = value
            else:
                hops[name] = value
        hop_keys = list(hops)
        hops = dict(zip(hop_keys, lax.optimization_barrier([hops[n] for n in hop_keys])))

    gram = gram + dot_of([(1, 1), (3, 0), (2, 0), (2, 1)])

    rounded = gram.astype(jnp.bfloat16)
    member = member_of(sel_tiles, row_index, rows_here)
    product = dot_f32(coupling_full, rounded, ((0,), (1,)))
    product = jnp.where(member[None, :], -product, jnp.float32(0.0))
    out_rows = product.shape[0] // cols
    child = lax.dynamic_slice_in_dim(product, col_index * out_rows, out_rows, 0)
    for flip in range(1, cols):
        piece = lax.dynamic_slice_in_dim(product, (col_index ^ flip) * out_rows, out_rows, 0)
        moved = lax.ppermute(
            piece.astype(jnp.bfloat16), "col", [(c, c ^ flip) for c in range(cols)]
        )
        child = child + moved.astype(jnp.float32)
    return (gram, child)


def solution(mesh):
    square = mesh.shape["col"] == 4 and mesh.shape["row"] == CORES * mesh.shape["col"]
    placed = (P("row", "col"), P(), P("col", "row"))
    return jax.shard_map(
        square_body if square else general_body,
        mesh=mesh,
        in_specs=placed,
        out_specs=(P("row", "col"), P("col", "row")),
        check_vma=False,
    )
```
